32 devices in a mesh: depth: 4 (over y, x), screen: 8 (over z, core).
Axes of the slice: x: 2, y: 2, z: 4, core: 2. Of those that a mesh axis runs over, the one named last changes fastest.
Arguments:
- voxel_bins: int32 [32, 256, 2048], P('depth', None, 'screen'), may hold values from 0 to 255
- colors: bfloat16 [3, 256], replicated, may hold values from 0 to 2
- opacity: bfloat16 [256], replicated, may hold values from 0 to 1
- slab_order: int32 [8, 4], replicated, may hold values from 0 to 3, each once within a row
Outputs:
- image: float32 [4, 256, 2048], P(None, ('depth', 'screen'))
The draws below stay inside these ranges and needn't reach their ends.
Inputs may be any that keep to these rules, and one draw needn't show every extreme that they name: `slab_order`: every row is a permutation of 0 to 3.
All inputs are finite; a program needn't handle non-finite values.
Results may differ from the reference program's by a relative error of at most 0.0003.
Values sent between devices are 32-bit elements; how exact they have to be, the bound alone decides.
No kernel may reach another device: no remote copies, remote signals or barrier semaphores. Data moves between devices by JAX's collectives and lax.ppermute only.
A program may use at most 64 MiB of HBM per device.

```python
import jax
import jax.numpy as jnp
from jax import lax

NBINS = 256
IMG_H = 256
SAMPLES = 32
IMG_W = 2048
DEPTHS = 4
TILES = 8


def place_ends(result, own_key, least, largest):
    extent = result.shape
    index_at = [jax.random.randint(jax.random.fold_in(own_key, axis), (), 0, extent[axis]) for axis in range(len(extent))]
    result = result.at[tuple(index_at)].set(least)
    longest = extent.index(max(extent))
    index_at[longest] = (index_at[longest] + 1) % extent[longest]
    return result.at[tuple(index_at)].set(largest)


def setup_inputs(seed: int = 0) -> dict:
    arg_keys = jax.random.split(jax.random.key(seed), 5)
    voxel_bins = place_ends(jax.random.randint(arg_keys[0], (SAMPLES, IMG_H, IMG_W), 0, NBINS), jax.random.fold_in(arg_keys[0], 1), 0, NBINS - 1).astype(jnp.int32)
    colors = jnp.clip(jax.random.uniform(arg_keys[1], (3, NBINS), jnp.float32, 0.0, 2.0), 0.0, 2.0).astype(jnp.bfloat16)
    opacity = jnp.clip(jax.random.uniform(arg_keys[2], (NBINS,), jnp.float32, 0.0, 1.0), 0.0, 1.0).astype(jnp.bfloat16)
    slab_order = jax.vmap(lambda own: jax.random.permutation(own, DEPTHS))(jax.random.split(arg_keys[3], TILES)).reshape((TILES, DEPTHS)).astype(jnp.int32)
    return dict(voxel_bins=voxel_bins, colors=colors, opacity=opacity, slab_order=slab_order)


def reference(voxel_bins, colors, opacity, slab_order):
    table = jnp.concatenate([colors, opacity[None]], axis=0).astype(jnp.float32)
    sample_total = voxel_bins.shape[0]
    slab_count = slab_order.shape[1]
    tile_count = slab_order.shape[0]
    row_count = voxel_bins.shape[1]
    col_count = voxel_bins.shape[2]
    extinct_rate = 3.0 / sample_total
    slabs = voxel_bins.reshape(slab_count, sample_total // slab_count, row_count, col_count)

    def march(slab):
        def advance(carried, layer):
            passed, color_sum = carried
            values = jnp.take(table, layer, axis=1)
            density = values[3]
            weight = (1.0 - jnp.exp(-extinct_rate * density)) * jnp.exp(-extinct_rate * passed)
            return (passed + density, color_sum + weight[None] * values[:3]), None

        start = (jnp.zeros((row_count, col_count), jnp.float32), jnp.zeros((3, row_count, col_count), jnp.float32))
        (passed, color_sum), ignored = lax.scan(advance, start, slab)
        final_alpha = 1.0 - jnp.exp(-extinct_rate * passed)
        return jnp.concatenate([color_sum, final_alpha[None]], axis=0)

    partials = lax.map(march, slabs)
    pieces = partials.reshape(slab_count, 4, row_count, tile_count, col_count // tile_count)
    acc_color = jnp.zeros((3, row_count, tile_count, col_count // tile_count), jnp.float32)
    acc_alpha = jnp.zeros((row_count, tile_count, col_count // tile_count), jnp.float32)
    for place in range(slab_count):
        select = (slab_order == place).astype(jnp.float32)
        picked = jnp.einsum("ti,icrtw->crtw", select, pieces, precision=lax.Precision.HIGHEST)
        acc_color = acc_color + (1.0 - acc_alpha)[None] * picked[:3]
        acc_alpha = acc_alpha + (1.0 - acc_alpha) * picked[3]
    merged = jnp.concatenate([acc_color, acc_alpha[None]], axis=0)
    return merged.reshape(4, row_count, col_count)
```

```python
import functools

import jax
import jax.numpy as jnp
from jax import lax
from jax.experimental import pallas as pl
from jax.experimental.pallas import tpu as pltpu
from jax.sharding import PartitionSpec as P

extinction = 3.0
lanes = 128
sublanes = 8


def partner_of(index, step, count):
    if count & (count - 1) == 0:
        return index ^ step
    return (index + step) % count


def source_of(index, step, count):
    if count & (count - 1) == 0:
        return index ^ step
    return (index - step) % count


def render_kernel(block_ref, colors_ref, opacity_ref, bins_ref, out_ref, *, rate):
    samples_here, row_count, col_count = bins_ref.shape
    clear = jnp.exp(-rate * opacity_ref[...].astype(jnp.float32))
    shade = (1.0 - clear) * colors_ref[...].astype(jnp.float32)
    full = jnp.concatenate([shade, clear], axis=0)
    bin_count = full.shape[1]
    halves = bin_count // lanes
    tables = [
        [
            jnp.broadcast_to(full[c : c + 1, h * lanes : (h + 1) * lanes], (sublanes, lanes))
            for h in range(halves)
        ]
        for c in range(4)
    ]

    def advance(group, ignored):
        rows = pl.ds(pl.multiple_of(group * sublanes, sublanes), sublanes)
        for col in range(0, col_count, lanes):
            cols = slice(col, col + lanes)
            for sample in range(samples_here):
                index = bins_ref[sample, rows, cols]
                low = index & (lanes - 1)
                high = index // lanes if halves > 2 else index >= lanes
                picked = []
                for c in range(4):
                    value = jnp.take_along_axis(tables[c][0], low, axis=1, mode="promise_in_bounds")
                    for h in range(1, halves):
                        other = jnp.take_along_axis(
                            tables[c][h], low, axis=1, mode="promise_in_bounds"
                        )
                        value = jnp.where(high if halves == 2 else high == h, other, value)
                    picked.append(value)
                if sample == 0:
                    sums = picked[:3]
                    through = picked[3]
                else:
                    sums = [s + through * v for s, v in zip(sums, picked[:3])]
                    through = through * picked[3]
            for c in range(3):
                out_ref[c, rows, cols] = sums[c]
            out_ref[3, rows, cols] = 1.0 - through
        return ignored

    lax.fori_loop(0, row_count // sublanes, advance, 0)


def render_block(voxel_bins, colors, opacity_row, block, block_rows, rate):
    samples_here, row_count, col_count = voxel_bins.shape
    steps = 2 if block_rows % (2 * sublanes) == 0 else 1
    step_rows = block_rows // steps
    return pl.pallas_call(
        functools.partial(render_kernel, rate=rate),
        out_shape=pltpu.VMEM((4, block_rows, col_count), jnp.float32),
        grid_spec=pltpu.PrefetchScalarGridSpec(
            num_scalar_prefetch=1,
            grid=(steps,),
            in_specs=[
                pl.BlockSpec(colors.shape, lambda i, b: (0, 0)),
                pl.BlockSpec(opacity_row.shape, lambda i, b: (0, 0)),
                pl.BlockSpec(
                    (samples_here, step_rows, col_count), lambda i, b: (0, b[0] * steps + i, 0)
                ),
            ],
            out_specs=pl.BlockSpec((4, step_rows, col_count), lambda i, b: (0, i, 0)),
        ),
        compiler_params=pltpu.CompilerParams(dimension_semantics=("arbitrary",)),
        name="render_block",
    )(block, colors, opacity_row, voxel_bins)


def composite_kernel(places_ref, *refs):
    pieces, out_ref = refs[:-1], refs[-1]
    count = len(pieces)
    target_count, ignored, owned_rows, col_count = out_ref.shape
    together = max(1, sublanes // owned_rows)
    group_rows = together * owned_rows

    def advance(group, ignored):
        rows = pl.ds(pl.multiple_of(group * group_rows, group_rows), group_rows)

        def put(channel, value):
            for i in range(together):
                out_ref[group * together + i, channel] = value[
                    i * owned_rows : (i + 1) * owned_rows
                ]

        clear = [1.0 - piece[3, rows, :] for piece in pieces]
        before = [None] * count
        for j in range(count):
            for k in range(j + 1, count):
                first = places_ref[j] < places_ref[k]
                onto_k = jnp.where(first, clear[j], 1.0)
                onto_j = jnp.where(first, 1.0, clear[k])
                before[k] = onto_k if before[k] is None else before[k] * onto_k
                before[j] = onto_j if before[j] is None else before[j] * onto_j
        for c in range(3):
            total = before[0] * pieces[0][c, rows, :]
            for j in range(1, count):
                total = total + before[j] * pieces[j][c, rows, :]
            put(c, total)
        through = clear[0]
        for j in range(1, count):
            through = through * clear[j]
        put(3, 1.0 - through)
        return ignored

    lax.fori_loop(0, target_count // together, advance, 0)


def composite(pieces, places, target_count):
    channels, block_rows, col_count = pieces[0].shape
    return pl.pallas_call(
        composite_kernel,
        out_shape=pltpu.VMEM(
            (target_count, 4, block_rows // target_count, col_count), jnp.float32
        ),
        in_specs=[pl.BlockSpec(memory_space=pltpu.SMEM)]
        + [pl.BlockSpec(memory_space=pltpu.VMEM)] * len(pieces),
        out_specs=pl.BlockSpec(memory_space=pltpu.VMEM),
        name="composite",
    )(places, *[pltpu.with_memory_space_constraint(p, pltpu.VMEM) for p in pieces])


def assemble_kernel(tiles_ref, *refs):
    parts, out_ref = refs[:-1], refs[-1]
    col_count = parts[0].shape[-1]
    for i, part in enumerate(parts):
        cols = pl.ds(pl.multiple_of(tiles_ref[i] * col_count, col_count), col_count)
        out_ref[:, :, cols] = part[...]


def assemble(parts, tiles):
    channels, owned_rows, col_count = parts[0].shape
    return pl.pallas_call(
        assemble_kernel,
        out_shape=jax.ShapeDtypeStruct(
            (channels, owned_rows, col_count * len(parts)), jnp.float32
        ),
        in_specs=[pl.BlockSpec(memory_space=pltpu.SMEM)]
        + [pl.BlockSpec(memory_space=pltpu.VMEM)] * len(parts),
        out_specs=pl.BlockSpec(memory_space=pltpu.VMEM),
        name="assemble",
    )(tiles, *[pltpu.with_memory_space_constraint(p, pltpu.VMEM) for p in parts])


def local(voxel_bins, colors, opacity, slab_order):
    depth_count = lax.axis_size("depth")
    screen_count = lax.axis_size("screen")
    samples_here, row_count, col_count = voxel_bins.shape
    rate = extinction / (samples_here * depth_count)
    depth_index = lax.axis_index("depth")
    screen_index = lax.axis_index("screen")
    block_rows = row_count // depth_count
    opacity_row = opacity[None]

    pieces = [None] * depth_count
    for step in list(range(depth_count - 1, 0, -1)) + [0]:
        block = partner_of(depth_index, step, depth_count).astype(jnp.int32)[None]
        piece = render_block(voxel_bins, colors, opacity_row, block, block_rows, rate)
        if step:
            pairs = [(i, partner_of(i, step, depth_count)) for i in range(depth_count)]
            piece = lax.ppermute(piece, "depth", pairs)
        pieces[step] = piece
    own_order = lax.dynamic_index_in_dim(slab_order, screen_index, 0, keepdims=False)
    sources = jnp.stack([source_of(depth_index, step, depth_count) for step in range(depth_count)])
    places = own_order[sources]
    blocks = composite(pieces, places, screen_count)
    parts = [lax.dynamic_index_in_dim(blocks, screen_index, 0, keepdims=False)]
    for step in range(1, screen_count):
        target = partner_of(screen_index, step, screen_count)
        pairs = [(i, partner_of(i, step, screen_count)) for i in range(screen_count)]
        part = lax.dynamic_index_in_dim(blocks, target, 0, keepdims=False)
        parts.append(lax.ppermute(part, "screen", pairs))
    tiles = jnp.stack([source_of(screen_index, step, screen_count) for step in range(screen_count)])
    return assemble(parts, tiles)


def solution(mesh):
    placed = (P("depth", None, "screen"), P(), P(), P())
    return jax.shard_map(
        local,
        mesh=mesh,
        in_specs=placed,
        out_specs=P(None, ("depth", "screen"), None),
        check_vma=False,
    )
```

```python
import functools

import jax
import jax.numpy as jnp
from jax import lax
from jax.experimental import pallas as pl
from jax.experimental.pallas import tpu as pltpu
from jax.sharding import PartitionSpec as P


extinction = 3.0
lanes = 128
sublanes = 8


def partner_of(index, step, count):
    if count & (count - 1) == 0:
        return index ^ step
    return (index + step) % count


def source_of(index, step, count):
    if count & (count - 1) == 0:
        return index ^ step
    return (index - step) % count


def in_vmem(array):
    return pltpu.with_memory_space_constraint(array, pltpu.VMEM)


def march(tables, bins_ref, first_row, out_ref):
    samples_here, _, col_count = bins_ref.shape
    row_count = out_ref.shape[1]
    halves = len(tables[0])
    groups = row_count // sublanes
    unrolled = 4 if groups % 4 == 0 else 1

    def advance(step, ignored):
        for inner in range(unrolled):
            row = pl.multiple_of((step * unrolled + inner) * sublanes, sublanes)
            to_rows = pl.ds(row, sublanes)
            rows = pl.ds(pl.multiple_of(first_row + row, sublanes), sublanes)
            for col in range(0, col_count, lanes):
                cols = slice(col, col + lanes)
                for sample in range(samples_here):
                    index = bins_ref[sample, rows, cols]
                    low = index & (lanes - 1)
                    high = index // lanes if halves > 2 else index >= lanes
                    picked = []
                    for c in range(4):
                        value = jnp.take_along_axis(
                            tables[c][0], low, axis=1, mode="promise_in_bounds"
                        )
                        for h in range(1, halves):
                            other = jnp.take_along_axis(
                                tables[c][h], low, axis=1, mode="promise_in_bounds"
                            )
                            value = jnp.where(high if halves == 2 else high == h, other, value)
                        picked.append(value)
                    if sample == 0:
                        sums = picked[:3]
                        through = picked[3]
                    else:
                        sums = [s + through * v for s, v in zip(sums, picked[:3])]
                        through = through * picked[3]
                for c in range(3):
                    out_ref[c, to_rows, cols] = sums[c]
                out_ref[3, to_rows, cols] = 1.0 - through
        return ignored

    lax.fori_loop(0, groups // unrolled, advance, 0)


def render_kernel(colors_hbm, opacity_hbm, bins_hbm, *refs, steps, rate):
    out_refs = refs[:-5]
    colors_ref, opacity_ref, bins_ref, bins_sems, table_sems = refs[-5:]
    block_rows = out_refs[0].shape[1]
    depth_count = lax.axis_size("depth")
    depth_index = lax.axis_index("depth")
    small = [
        pltpu.make_async_copy(colors_hbm, colors_ref, table_sems.at[0]),
        pltpu.make_async_copy(opacity_hbm, opacity_ref, table_sems.at[1]),
    ]
    for copy in small:
        copy.start()
    copies = []
    for i, step in enumerate(steps):
        first_row = partner_of(depth_index, step, depth_count) * block_rows
        rows = pl.ds(pl.multiple_of(first_row, block_rows), block_rows)
        to_rows = pl.ds(i * block_rows, block_rows)
        copies.append(
            pltpu.make_async_copy(bins_hbm.at[:, rows], bins_ref.at[:, to_rows], bins_sems.at[i])
        )
        copies[-1].start()
    for copy in small:
        copy.wait()
    opacity = opacity_ref[...].astype(jnp.float32).reshape(1, -1)
    clear = jnp.exp(-rate * opacity)
    shade = (1.0 - clear) * colors_ref[...].astype(jnp.float32)
    full = jnp.concatenate([shade, clear], axis=0)
    tables = [
        [
            jnp.broadcast_to(full[c : c + 1, h : h + lanes], (sublanes, lanes))
            for h in range(0, full.shape[1], lanes)
        ]
        for c in range(4)
    ]
    for i, copy in enumerate(copies):
        copy.wait()
        march(tables, bins_ref, i * block_rows, out_refs[i])


def smem_spec():
    return pl.BlockSpec(memory_space=pltpu.SMEM)


def vmem_spec():
    return pl.BlockSpec(memory_space=pltpu.VMEM)


def render(voxel_bins, colors, opacity, steps, block_rows, rate):
    samples_here, _, col_count = voxel_bins.shape
    return pl.pallas_call(
        functools.partial(render_kernel, steps=steps, rate=rate),
        out_shape=[pltpu.VMEM((4, block_rows, col_count), jnp.float32)] * len(steps),
        in_specs=[pl.BlockSpec(memory_space=pl.ANY)] * 3,
        out_specs=[vmem_spec()] * len(steps),
        scratch_shapes=[
            pltpu.VMEM(colors.shape, colors.dtype),
            pltpu.VMEM(opacity.shape, opacity.dtype),
            pltpu.VMEM((samples_here, len(steps) * block_rows, col_count), voxel_bins.dtype),
            pltpu.SemaphoreType.DMA((len(steps),)),
            pltpu.SemaphoreType.DMA((2,)),
        ],
        name="render",
    )(colors, opacity, voxel_bins)


def composite_kernel(order_ref, *refs):
    pieces, out_ref = refs[:-1], refs[-1]
    count = len(pieces)
    depth_index = lax.axis_index("depth")
    screen_index = lax.axis_index("screen")
    places = [
        order_ref[screen_index, source_of(depth_index, step, count)] for step in range(count)
    ]
    target_count, _, owned_rows, _ = out_ref.shape
    together = max(1, sublanes // owned_rows)
    group_rows = together * owned_rows

    def advance(group, ignored):
        rows = pl.ds(pl.multiple_of(group * group_rows, group_rows), group_rows)

        def put(channel, value):
            for i in range(together):
                out_ref[group * together + i, channel] = value[
                    i * owned_rows : (i + 1) * owned_rows
                ]

        clear = [1.0 - piece[3, rows, :] for piece in pieces]
        before = [None] * count
        for j in range(count):
            for k in range(j + 1, count):
                first = places[j] < places[k]
                onto_k = jnp.where(first, clear[j], 1.0)
                onto_j = jnp.where(first, 1.0, clear[k])
                before[k] = onto_k if before[k] is None else before[k] * onto_k
                before[j] = onto_j if before[j] is None else before[j] * onto_j
        for c in range(3):
            total = before[0] * pieces[0][c, rows, :]
            for j in range(1, count):
                total = total + before[j] * pieces[j][c, rows, :]
            put(c, total)
        through = clear[0]
        for j in range(1, count):
            through = through * clear[j]
        put(3, 1.0 - through)
        return ignored

    lax.fori_loop(0, target_count // together, advance, 0)


def composite(pieces, slab_order, target_count):
    _, block_rows, col_count = pieces[0].shape
    return pl.pallas_call(
        composite_kernel,
        out_shape=pltpu.VMEM(
            (target_count, 4, block_rows // target_count, col_count), jnp.float32
        ),
        in_specs=[smem_spec()] + [vmem_spec()] * len(pieces),
        out_specs=vmem_spec(),
        name="composite",
    )(slab_order, *[in_vmem(piece) for piece in pieces])


def assemble_kernel(*refs, steps):
    parts, out_ref, sems = refs[:-2], refs[-2], refs[-1]
    col_count = parts[0].shape[-1]
    screen_count = lax.axis_size("screen")
    screen_index = lax.axis_index("screen")
    copies = []
    for i, part in enumerate(parts):
        tile = source_of(screen_index, steps[i], screen_count)
        cols = pl.ds(pl.multiple_of(tile * col_count, col_count), col_count)
        copies.append(pltpu.make_async_copy(part, out_ref.at[:, :, cols], sems.at[i]))
        copies[-1].start()
    for copy in copies:
        copy.wait()


def assemble(parts, steps):
    channels, owned_rows, col_count = parts[0].shape
    return pl.pallas_call(
        functools.partial(assemble_kernel, steps=steps),
        out_shape=jax.ShapeDtypeStruct(
            (channels, owned_rows, col_count * len(parts)), jnp.float32
        ),
        in_specs=[vmem_spec()] * len(parts),
        out_specs=pl.BlockSpec(memory_space=pl.ANY),
        scratch_shapes=[pltpu.SemaphoreType.DMA((len(parts),))],
        name="assemble",
    )(*[in_vmem(part) for part in parts])


def local(voxel_bins, colors, opacity, slab_order):
    depth_count = lax.axis_size("depth")
    screen_count = lax.axis_size("screen")
    samples_here, row_count, _ = voxel_bins.shape
    rate = extinction / (samples_here * depth_count)
    screen_index = lax.axis_index("screen")
    block_rows = row_count // depth_count
    pieces = [None] * depth_count
    for steps in ((1, 2), tuple(range(3, depth_count)), (0,)):
        rendered = render(voxel_bins, colors, opacity, steps, block_rows, rate)
        for step, piece in zip(steps, rendered):
            if step:
                pairs = [(i, partner_of(i, step, depth_count)) for i in range(depth_count)]
                piece = lax.ppermute(piece, "depth", pairs)
            pieces[step] = piece
    blocks = composite(pieces, slab_order, screen_count)
    parts = []
    steps = list(range(screen_count - 1, 0, -1)) + [0]
    for step in steps:
        target = partner_of(screen_index, step, screen_count)
        part = lax.dynamic_index_in_dim(blocks, target, 0, keepdims=False)
        if step:
            pairs = [(i, partner_of(i, step, screen_count)) for i in range(screen_count)]
            part = lax.ppermute(part, "screen", pairs)
        parts.append(part)
    return assemble(parts, tuple(steps))


def solution(mesh):
    placed = (P("depth", None, "screen"), P(), P(), P())
    return jax.shard_map(
        local,
        mesh=mesh,
        in_specs=placed,
        out_specs=P(None, ("depth", "screen"), None),
        check_vma=False,
    )
```

```python
import functools

import jax
import jax.numpy as jnp
from jax import lax
from jax.experimental import pallas as pl
from jax.experimental.pallas import tpu as pltpu
from jax.sharding import PartitionSpec as P


extinction = 3.0
lanes = 128
sublanes = 8


def partner_of(index, step, count):
    if count & (count - 1) == 0:
        return index ^ step
    return (index + step) % count


def source_of(index, step, count):
    if count & (count - 1) == 0:
        return index ^ step
    return (index - step) % count


def in_vmem(array):
    return pltpu.with_memory_space_constraint(array, pltpu.VMEM)


def march(tables, bins_ref, row, col):
    halves = len(tables[0])
    rows = pl.ds(row, sublanes)
    cols = slice(col, col + lanes)
    for sample in range(bins_ref.shape[0]):
        index = bins_ref[sample, rows, cols]
        low = index & (lanes - 1)
        high = index // lanes if halves > 2 else index >= lanes
        picked = []
        for c in range(4):
            value = jnp.take_along_axis(tables[c][0], low, axis=1, mode="promise_in_bounds")
            for h in range(1, halves):
                other = jnp.take_along_axis(tables[c][h], low, axis=1, mode="promise_in_bounds")
                value = jnp.where(high if halves == 2 else high == h, other, value)
            picked.append(value)
        if sample == 0:
            sums = picked[:3]
            through = picked[3]
        else:
            sums = [s + through * v for s, v in zip(sums, picked[:3])]
            through = through * picked[3]
    return sums + [1.0 - through]


def march_block(tables, bins_ref, first_row, same_ref, other_ref, parity):
    pair_count, _, owned_rows, col_count = same_ref.shape
    outs = (same_ref, other_ref)

    def whole_groups(pair):
        for flip in range(2):
            target = 2 * pair + (parity ^ flip)
            for sub in range(0, owned_rows, sublanes):
                row = pl.multiple_of(first_row + target * owned_rows + sub, sublanes)
                for col in range(0, col_count, lanes):
                    values = march(tables, bins_ref, row, col)
                    for c in range(4):
                        outs[flip][pair, c, sub : sub + sublanes, col : col + lanes] = values[c]

    def shared_group(group):
        row = pl.multiple_of(first_row + group * sublanes, sublanes)
        pairs = sublanes // (2 * owned_rows)
        for col in range(0, col_count, lanes):
            values = march(tables, bins_ref, row, col)
            for c in range(4):
                for i in range(pairs):
                    start = 2 * i * owned_rows
                    even = values[c][start : start + owned_rows]
                    odd = values[c][start + owned_rows : start + 2 * owned_rows]
                    where = (group * pairs + i, c, slice(None), slice(col, col + lanes))
                    same_ref[where] = jnp.where(parity == 0, even, odd)
                    other_ref[where] = jnp.where(parity == 0, odd, even)

    if owned_rows % sublanes == 0:
        visit, count = whole_groups, pair_count
    else:
        visit, count = shared_group, 2 * pair_count * owned_rows // sublanes
    unrolled = 2 if count % 2 == 0 else 1

    def advance(step, ignored):
        for inner in range(unrolled):
            visit(step * unrolled + inner)
        return ignored

    lax.fori_loop(0, count // unrolled, advance, 0)


def render_kernel(colors_hbm, opacity_hbm, bins_hbm, *refs, steps, rate):
    out_refs = refs[:-5]
    colors_ref, opacity_ref, bins_ref, bins_sems, table_sems = refs[-5:]
    pair_count, ignored, owned_rows, ignored = out_refs[0].shape
    block_rows = 2 * pair_count * owned_rows
    parity = lax.axis_index("screen") % 2
    depth_count = lax.axis_size("depth")
    depth_index = lax.axis_index("depth")
    small = [
        pltpu.make_async_copy(colors_hbm, colors_ref, table_sems.at[0]),
        pltpu.make_async_copy(opacity_hbm, opacity_ref, table_sems.at[1]),
    ]
    for copy in small:
        copy.start()
    copies = []
    for i, step in enumerate(steps):
        first_row = partner_of(depth_index, step, depth_count) * block_rows
        rows = pl.ds(pl.multiple_of(first_row, block_rows), block_rows)
        to_rows = pl.ds(i * block_rows, block_rows)
        copies.append(
            pltpu.make_async_copy(bins_hbm.at[:, rows], bins_ref.at[:, to_rows], bins_sems.at[i])
        )
        copies[-1].start()
    for copy in small:
        copy.wait()
    opacity = opacity_ref[...].astype(jnp.float32).reshape(1, -1)
    clear = jnp.exp(-rate * opacity)
    shade = (1.0 - clear) * colors_ref[...].astype(jnp.float32)
    full = jnp.concatenate([shade, clear], axis=0)
    tables = [
        [
            jnp.broadcast_to(full[c : c + 1, h : h + lanes], (sublanes, lanes))
            for h in range(0, full.shape[1], lanes)
        ]
        for c in range(4)
    ]
    for i, copy in enumerate(copies):
        copy.wait()
        march_block(
            tables, bins_ref, i * block_rows, out_refs[2 * i], out_refs[2 * i + 1], parity
        )


def smem_spec():
    return pl.BlockSpec(memory_space=pltpu.SMEM)


def vmem_spec():
    return pl.BlockSpec(memory_space=pltpu.VMEM)


def render(voxel_bins, colors, opacity, steps, piece_shape, block_rows, rate):
    samples_here, _, col_count = voxel_bins.shape
    return pl.pallas_call(
        functools.partial(render_kernel, steps=steps, rate=rate),
        out_shape=[pltpu.VMEM(piece_shape, jnp.float32)] * (2 * len(steps)),
        in_specs=[pl.BlockSpec(memory_space=pl.ANY)] * 3,
        out_specs=[vmem_spec()] * (2 * len(steps)),
        scratch_shapes=[
            pltpu.VMEM(colors.shape, colors.dtype),
            pltpu.VMEM(opacity.shape, opacity.dtype),
            pltpu.VMEM((samples_here, len(steps) * block_rows, col_count), voxel_bins.dtype),
            pltpu.SemaphoreType.DMA((len(steps),)),
            pltpu.SemaphoreType.DMA((2,)),
        ],
        name="render",
    )(colors, opacity, voxel_bins)


def composite_kernel(order_ref, *refs):
    pieces, out_ref = refs[:-1], refs[-1]
    count = len(pieces) // 2
    col_count = out_ref.shape[3] // 2
    depth_index = lax.axis_index("depth")
    screen_index = lax.axis_index("screen")

    def advance(target, ignored):
        for side, tile in enumerate((screen_index, screen_index ^ 1)):
            own = pieces[side * count : (side + 1) * count]
            places = [
                order_ref[tile, source_of(depth_index, step, count)] for step in range(count)
            ]
            cols = pl.ds(pl.multiple_of((tile % 2) * col_count, col_count), col_count)
            clear = [1.0 - piece[target, 3] for piece in own]
            before = [None] * count
            for j in range(count):
                for k in range(j + 1, count):
                    first = places[j] < places[k]
                    onto_k = jnp.where(first, clear[j], 1.0)
                    onto_j = jnp.where(first, 1.0, clear[k])
                    before[k] = onto_k if before[k] is None else before[k] * onto_k
                    before[j] = onto_j if before[j] is None else before[j] * onto_j
            for c in range(3):
                total = before[0] * own[0][target, c]
                for j in range(1, count):
                    total = total + before[j] * own[j][target, c]
                out_ref[target, c, :, cols] = total
            through = clear[0]
            for j in range(1, count):
                through = through * clear[j]
            out_ref[target, 3, :, cols] = 1.0 - through
        return ignored

    lax.fori_loop(0, out_ref.shape[0], advance, 0)


def composite(pieces, slab_order):
    pair_count, channels, owned_rows, col_count = pieces[0].shape
    return pl.pallas_call(
        composite_kernel,
        out_shape=pltpu.VMEM((pair_count, channels, owned_rows, 2 * col_count), jnp.float32),
        in_specs=[smem_spec()] + [vmem_spec()] * len(pieces),
        out_specs=vmem_spec(),
        name="composite",
    )(slab_order, *[in_vmem(piece) for piece in pieces])


def assemble_kernel(*refs, steps):
    parts, out_ref, sems = refs[:-2], refs[-2], refs[-1]
    col_count = parts[0].shape[-1]
    pair_count = lax.axis_size("screen") // 2
    pair_index = lax.axis_index("screen") // 2
    copies = []
    for i, part in enumerate(parts):
        tile = source_of(pair_index, steps[i], pair_count)
        cols = pl.ds(pl.multiple_of(tile * col_count, col_count), col_count)
        copies.append(pltpu.make_async_copy(part, out_ref.at[:, :, cols], sems.at[i]))
        copies[-1].start()
    for copy in copies:
        copy.wait()


def assemble(parts, steps):
    channels, owned_rows, col_count = parts[0].shape
    return pl.pallas_call(
        functools.partial(assemble_kernel, steps=steps),
        out_shape=jax.ShapeDtypeStruct(
            (channels, owned_rows, col_count * len(parts)), jnp.float32
        ),
        in_specs=[vmem_spec()] * len(parts),
        out_specs=pl.BlockSpec(memory_space=pl.ANY),
        scratch_shapes=[pltpu.SemaphoreType.DMA((len(parts),))],
        name="assemble",
    )(*[in_vmem(part) for part in parts])


def local(voxel_bins, colors, opacity, slab_order):
    depth_count = lax.axis_size("depth")
    screen_count = lax.axis_size("screen")
    samples_here, row_count, col_count = voxel_bins.shape
    rate = extinction / (samples_here * depth_count)
    block_rows = row_count // depth_count
    pair_count = screen_count // 2
    piece_shape = (pair_count, 4, block_rows // screen_count, col_count)

    def exchange(piece, step, flip):
        pairs = [
            (
                d * screen_count + s,
                partner_of(d, step, depth_count) * screen_count + (s ^ flip),
            )
            for d in range(depth_count)
            for s in range(screen_count)
        ]
        return lax.ppermute(piece, ("depth", "screen"), pairs)

    same = [None] * depth_count
    other = [None] * depth_count
    for steps in ((1, 2), tuple(range(3, depth_count)), (0,)):
        rendered = render(voxel_bins, colors, opacity, steps, piece_shape, block_rows, rate)
        for i, step in enumerate(steps):
            same[step] = exchange(rendered[2 * i], step, 0) if step else rendered[2 * i]
            other[step] = exchange(rendered[2 * i + 1], step, 1)
    blocks = composite(same + other, slab_order)
    parts = []
    steps = list(range(pair_count - 1, 0, -1)) + [0]
    for step in steps:
        target = partner_of(lax.axis_index("screen") // 2, step, pair_count)
        part = lax.dynamic_index_in_dim(blocks, target, 0, keepdims=False)
        if step:
            pairs = [
                (s, partner_of(s // 2, step, pair_count) * 2 + s % 2) for s in range(screen_count)
            ]
            part = lax.ppermute(part, "screen", pairs)
        parts.append(part)
    return assemble(parts, tuple(steps))


def solution(mesh):
    placed = (P("depth", None, "screen"), P(), P(), P())
    return jax.shard_map(
        local,
        mesh=mesh,
        in_specs=placed,
        out_specs=P(None, ("depth", "screen"), None),
        check_vma=False,
    )
```
